32 devices in a mesh: fsdp: 8 (over z, x), grp: 4 (over y, core).
Axes of the slice: x: 2, y: 2, z: 4, core: 2. Of those that a mesh axis runs over, the one named last changes fastest.
Arguments:
- grad: bfloat16 [28672, 8192], P('fsdp', 'grp'), may hold values from -6 to 6
- projector_t: bfloat16 [1024, 8192], P('fsdp', 'grp'), may hold values from -0.0625 to 0.0625
- first_moment: float32 [28672, 1024], P('fsdp', 'grp'), may hold values from -3 to 3
- second_moment: float32 [28672, 1024], P('fsdp', 'grp'), may hold values from 0.0001 to 0.01
Outputs:
- update: float32 [28672, 8192], P('fsdp', 'grp')
- first_new: float32 [28672, 1024], P('fsdp', 'grp')
- second_new: float32 [28672, 1024], P('fsdp', 'grp')
The draws below stay inside these ranges and needn't reach their ends.
All inputs are finite; a program needn't handle non-finite values.
Results may differ from the reference program's by a relative error of at most 0.0029.
Values may be sent and summed in bfloat16 or wider, within the bound.
A program may use at most 128 MiB of HBM per device.

```python
import math
import jax
import jax.numpy as jnp
from jax import lax

M = 8192
N = 28672
R = 1024
STEP = 10


def steps_of(own_key, extent, split, least, largest):
    level = 1.0
    for axis_at, parts in split:
        draws = jax.random.uniform(jax.random.fold_in(jax.random.fold_in(own_key, 6), axis_at), (parts,), jnp.float32, least / len(split), largest / len(split))
        level = level * jnp.repeat(jnp.exp(draws), extent[axis_at] // parts).reshape((-1,) + (1,) * (len(extent) - 1 - axis_at))
    return level


def centred(rng, dims, spread, most, cuts=(), held_as=jnp.bfloat16):
    values = spread * jax.random.normal(rng, dims, jnp.float32)
    if cuts:
        values = values * steps_of(rng, dims, cuts, -0.22, 0.18)
    return jnp.clip(values, -most, most).astype(held_as)


def setup_inputs(seed: int = 0) -> dict:
    splits = jax.random.split(jax.random.key(seed), 5)
    return {
        "grad": centred(splits[0], (N, M), 1.0, 6.0, ((0, 8), (1, 4))),
        "projector_t": centred(splits[1], (R, M), M ** -0.5, 0.0625, ((0, 8), (1, 4))),
        "first_moment": centred(splits[2], (N, R), 0.5, 3.0, ((0, 8), (1, 4)), jnp.float32),
        "second_moment": jnp.clip(jnp.exp(math.log(0.01) - 4.6051702 * jax.random.uniform(splits[3], (N, R), jnp.float32) ** steps_of(splits[3], (N, R), ((0, 8), (1, 4)), -0.2, 0.2)), 0.0001, 0.01),
    }


def reference(grad, projector_t, first_moment, second_moment):
    projected = lax.dot_general(grad, projector_t, (((1,), (1,)), ((), ())), preferred_element_type=jnp.float32)
    first_new = 0.9 * first_moment + 0.1 * projected
    second_new = 0.999 * second_moment + 0.001 * projected * projected
    correct_one = 1.0 - 0.9 ** STEP
    correct_two = 1.0 - 0.999 ** STEP
    normalized = (first_new / correct_one / (jnp.sqrt(second_new / correct_two) + 1e-08)).astype(jnp.bfloat16)
    update = jnp.dot(normalized, projector_t, preferred_element_type=jnp.float32)
    return (update, first_new, second_new)
```

```python
import functools
import jax
import jax.numpy as jnp
from jax import lax
from jax.experimental import pallas as pl
from jax.experimental.pallas import tpu as pltpu
from jax.sharding import PartitionSpec as P

STEP = 10
CORRECT_ONE = 1.0 - 0.9**STEP
CORRECT_TWO = 1.0 - 0.999**STEP
MESH = pl.DeviceIdType.MESH
LANES = 128
VMEM_LIMIT = 63 << 20


def flips(size):
    width = size.bit_length() - 1
    return [int(format(p, "b").zfill(width)[::-1], 2) if width else 0 for p in range(size)]


def swap(value, size, bit):
    return lax.ppermute(value, "grp", [(i, i ^ bit) for i in range(size)])


def pieces(rows):
    for count in (4, 2):
        if rows % (count * 8) == 0:
            return count
    return 1


def adam(total, first, second):
    one = 0.9 * first + 0.1 * total
    two = 0.999 * second + 0.001 * total * total
    return one, two


def normal(one, two):
    return (one / CORRECT_ONE / (jnp.sqrt(two / CORRECT_TWO) + 1e-08)).astype(jnp.bfloat16)


def plain_body(size, grad, projector_t, first_moment, second_moment):
    me = lax.axis_index("grp")
    whole = lax.all_gather(projector_t, "fsdp", axis=0, tiled=True)
    block = whole.shape[0] // size
    ranked = jnp.concatenate(
        [lax.dynamic_slice_in_dim(whole, (me ^ flip) * block, block, 0) for flip in flips(size)]
    )
    ranked = lax.optimization_barrier(ranked)
    rows = grad.shape[0]
    count = pieces(rows)
    step = rows // count
    bits = [1 << b for b in range(size.bit_length() - 1)]
    update = jnp.zeros((rows, grad.shape[1]), jnp.float32)
    first_new = jnp.zeros(first_moment.shape, jnp.float32)
    second_new = jnp.zeros(second_moment.shape, jnp.float32)
    for c in range(count):
        at = c * step
        part = lax.slice_in_dim(grad, at, at + step)
        half = ranked.shape[0] // 2
        total = None
        for n, bit in enumerate(bits):
            if n == 0:
                away = lax.dot_general(
                    part, ranked[half:], (((1,), (1,)), ((), ())), preferred_element_type=jnp.float32
                ).astype(jnp.bfloat16)
                total = lax.dot_general(
                    part, ranked[:half], (((1,), (1,)), ((), ())), preferred_element_type=jnp.float32
                )
            else:
                half = total.shape[1] // 2
                away = total[:, half:].astype(jnp.bfloat16)
                total = total[:, :half]
            total = total + swap(away, size, bit).astype(jnp.float32)
        one, two = adam(total, first_moment[at : at + step], second_moment[at : at + step])
        full = normal(one, two)
        first_new = lax.dynamic_update_slice_in_dim(first_new, one, at, 0)
        second_new = lax.dynamic_update_slice_in_dim(second_new, two, at, 0)
        for bit in reversed(bits):
            full = jnp.concatenate([full, swap(full, size, bit)], axis=1)
        out = jnp.dot(full, ranked, preferred_element_type=jnp.float32)
        update = lax.dynamic_update_slice_in_dim(update, out, at, 0)
    return (update, first_new, second_new)


def tile_of(rows, most):
    for t in range(most - most % 16, 0, -16):
        if rows % t == 0:
            return t
    return 0


def xor(a, b, bits):
    out = 0
    for i in range(bits):
        p = 1 << i
        out = out + ((a // p + b // p) % 2) * p
    return out


LAG_B, LAG_C, LAG_D, LAG_E = 2, 5, 8, 9
AHEAD = 3


def exchange_kernel(
    fsdp, tile,
    grad_hbm, proj_hbm, first_hbm, second_hbm,
    norm_hbm, total_hbm, whole_hbm,
    grad, whole, first, second, total, norm, away, near, cross, came,
    load_sem, grad_sem, mom_sem, out_sem,
    p_send, p_recv, d_send, d_recv, y_send, y_recv, ny_send, nd_send, n_recv,
):
    f = lax.axis_index("fsdp")
    g = lax.axis_index("grp")
    y, c = g // 2, g % 2
    shard = proj_hbm.shape[0]
    halves, rows, _ = total.shape
    stages = fsdp
    tiles = rows // tile
    bits = fsdp.bit_length() - 1
    steps = stages * tiles
    x_to = xor(f, 1, bits)
    core_to = y * 2 + (1 - c)
    y_to = (1 - y) * 2 + c

    def p_rows(sid):
        return whole.at[pl.ds(pl.multiple_of(sid * shard, shard), shard)]

    own = pltpu.make_async_copy(proj_hbm, p_rows(f), load_sem)
    own.start()

    def grad_copy(j):
        at = pl.ds(pl.multiple_of(j * tile, tile), tile)
        return pltpu.make_async_copy(grad_hbm.at[at], grad.at[at], grad_sem.at[j])

    def mom_copies():
        out = []
        for i, (src, dst) in enumerate(((first_hbm, first), (second_hbm, second))):
            for h in range(halves):
                out.append(
                    pltpu.make_async_copy(
                        src.at[:, pl.ds(h * shard, shard)], dst.at[h], mom_sem.at[i, h]
                    )
                )
        return out

    grad_copy(0).start()

    barrier = pltpu.get_barrier_semaphore()
    peers = [(xor(f, 1, bits), g), (f, core_to), (f, y_to)]
    peers += [(xor(f, 2 * m, bits), g) for m in range(1, fsdp // 2)]
    for peer in peers:
        pl.semaphore_signal(barrier, inc=1, device_id=peer, device_id_type=MESH)

    @pl.loop(1, tiles)
    def _(j):
        grad_copy(j).start()

    for copy in mom_copies():
        copy.start()
    pl.semaphore_wait(barrier, len(peers))
    own.wait()

    def p_copy(sid, to):
        return pltpu.make_async_remote_copy(
            p_rows(sid), p_rows(sid), p_send, p_recv.at[sid], device_id=(to, g), device_id_type=MESH
        )

    p_copy(f, x_to).start()
    for m in range(1, fsdp // 2):
        p_copy(f, xor(f, 2 * m, bits)).start()

    def place(s):
        k, j = s // tiles, s % tiles
        sid = xor(f, k, bits)
        block, h = sid // halves, sid % halves
        return k, pl.multiple_of(j * tile, tile), j, sid, block, h

    def product(sid, at):
        return lax.dot_general(
            grad[pl.ds(at, tile)],
            whole[pl.ds(pl.multiple_of(sid * shard, shard), shard)],
            (((1,), (1,)), ((), ())),
            preferred_element_type=jnp.float32,
        )

    def d_copy(slot, at, j):
        return pltpu.make_async_remote_copy(
            away.at[slot, pl.ds(at, tile)], near.at[slot, pl.ds(at, tile)], d_send, d_recv.at[slot, j],
            device_id=(f, core_to), device_id_type=MESH,
        )

    def y_copy(h, at, j):
        return pltpu.make_async_remote_copy(
            cross.at[h, pl.ds(at, tile)], came.at[h, pl.ds(at, tile)], y_send, y_recv.at[h, j],
            device_id=(f, y_to), device_id_type=MESH,
        )

    def n_copy(sid, at, j, send, to):
        ref = norm.at[sid, pl.ds(at, tile)]
        return pltpu.make_async_remote_copy(
            ref, ref, send, n_recv.at[sid, j], device_id=(f, to), device_id_type=MESH
        )

    def n_out(sid, at):
        return pltpu.make_async_copy(
            norm.at[sid, pl.ds(at, tile)], norm_hbm.at[sid, pl.ds(at, tile)], out_sem.at[0]
        )

    def whole_out():
        return pltpu.make_async_copy(whole, whole_hbm, out_sem.at[2])

    def step(t, carry):
        @pl.when(t < tiles)
        def _():
            grad_copy(t).wait()

        k = t // tiles

        @pl.when((t % tiles == 0) & (t < steps) & (k % 2 == 1))
        def _():
            sid = xor(f, k, bits)
            p_copy(sid, x_to).wait_recv()

        later = t + AHEAD

        @pl.when((later % (2 * tiles) == 0) & (later >= 2 * tiles) & (later < steps))
        def _():
            sid = xor(f, later // tiles, bits)
            p_copy(sid, x_to).wait_recv()
            p_copy(sid, x_to).start()

        @pl.when(t == steps - tiles)
        def _():
            whole_out().start()

        k, at, j, sid, block, h = place(t)

        @pl.when((t < steps) & (block % 2 != c))
        def _():
            slot = (block // 2) * halves + h
            away[slot, pl.ds(at, tile)] = product(sid, at).astype(jnp.bfloat16)
            d_copy(slot, at, j).start()

        s = t - LAG_B
        kb, atb, jb, sidb, blockb, hb = place(lax.max(s, 0))

        @pl.when((s >= 0) & (s < steps) & (blockb % 2 == c))
        def _():
            slot = (blockb // 2) * halves + hb
            part = product(sidb, atb)
            d_copy(slot, atb, jb).wait_recv()
            part = part + near[slot, pl.ds(atb, tile)].astype(jnp.float32)

            @pl.when(blockb // 2 != y)
            def _():
                cross[hb, pl.ds(atb, tile)] = part.astype(jnp.bfloat16)
                y_copy(hb, atb, jb).start()

            @pl.when(blockb // 2 == y)
            def _():
                total[hb, pl.ds(atb, tile)] = part

        s = t - LAG_C
        kc, atc, jc, sidc, blockc, hc = place(lax.max(s, 0))

        @pl.when(s == 0)
        def _():
            for copy in mom_copies():
                copy.wait()

        @pl.when((s >= 0) & (s < steps) & (blockc == g))
        def _():
            y_copy(hc, atc, jc).wait_recv()
            here = pl.ds(atc, tile)
            full = total[hc, here] + came[hc, here].astype(jnp.float32)
            total[hc, here] = full
            one, two = adam(full, first[hc, here], second[hc, here])
            norm[sidc, here] = normal(one, two)
            n_copy(sidc, atc, jc, ny_send, y_to).start()
            n_copy(sidc, atc, jc, nd_send, core_to).start()
            n_out(sidc, atc).start()
            pltpu.make_async_copy(total.at[hc, here], total_hbm.at[hc, here], out_sem.at[1]).start()

        s = t - LAG_D
        kd, atd, jd, sidd, blockd, hd = place(lax.max(s, 0))

        @pl.when((s >= 0) & (s < steps) & (blockd % 2 == c) & (blockd != g))
        def _():
            n_copy(sidd, atd, jd, nd_send, core_to).wait_recv()
            n_copy(sidd, atd, jd, nd_send, core_to).start()
            n_out(sidd, atd).start()

        s = t - LAG_E
        ke, ate, je, side, blocke, he = place(lax.max(s, 0))

        @pl.when((s >= 0) & (s < steps) & (blocke % 2 != c))
        def _():
            n_copy(side, ate, je, nd_send, core_to).wait_recv()
            n_out(side, ate).start()

        return carry

    lax.fori_loop(0, steps + LAG_E, step, 0)

    def sent(ref, sem):
        pltpu.make_async_remote_copy(
            ref, ref, sem, p_recv.at[0], device_id=(f, y_to), device_id_type=MESH
        ).wait_send()

    sent(whole.at[pl.ds(0, (fsdp - 1) * shard)], p_send)
    sent(away, d_send)
    sent(cross, y_send)
    sent(cross, ny_send)
    sent(away, nd_send)
    pltpu.make_async_copy(norm, norm_hbm, out_sem.at[0]).wait()
    pltpu.make_async_copy(total, total_hbm, out_sem.at[1]).wait()
    whole_out().wait()


def exchange(fsdp, tile, grad, projector_t, first, second):
    rows, depth = grad.shape
    shard = projector_t.shape[0]
    ranks = shard * fsdp
    block = first.shape[1]
    halves = block // shard
    tiles = rows // tile
    bf, fp = jnp.bfloat16, jnp.float32
    any_spec = pl.BlockSpec(memory_space=pl.ANY)
    sem = pltpu.SemaphoreType.DMA
    return pl.pallas_call(
        functools.partial(exchange_kernel, fsdp, tile),
        out_shape=(
            jax.ShapeDtypeStruct((fsdp, rows, shard), bf),
            jax.ShapeDtypeStruct((halves, rows, shard), fp),
            jax.ShapeDtypeStruct((ranks, depth), bf),
        ),
        in_specs=[any_spec] * 4,
        out_specs=(any_spec,) * 3,
        scratch_shapes=[
            pltpu.VMEM((rows, depth), bf),
            pltpu.VMEM((ranks, depth), bf),
            pltpu.VMEM((halves, rows, shard), fp),
            pltpu.VMEM((halves, rows, shard), fp),
            pltpu.VMEM((halves, rows, shard), fp),
            pltpu.VMEM((fsdp, rows, shard), bf),
            pltpu.VMEM((2 * halves, rows, shard), bf),
            pltpu.VMEM((2 * halves, rows, shard), bf),
            pltpu.VMEM((halves, rows, shard), bf),
            pltpu.VMEM((halves, rows, shard), bf),
            sem(()),
            sem((tiles,)),
            sem((2, halves)),
            sem((3,)),
            sem(()),
            sem((fsdp,)),
            sem(()),
            sem((2 * halves, tiles)),
            sem(()),
            sem((halves, tiles)),
            sem(()),
            sem(()),
            sem((fsdp, tiles)),
        ],
        compiler_params=pltpu.CompilerParams(
            collective_id=0, has_side_effects=True, vmem_limit_bytes=VMEM_LIMIT
        ),
        name="exchange",
    )(grad, projector_t, first, second)


def finish_kernel(norm, whole, total, first, second, update, first_new, second_new):
    full = jnp.concatenate([norm[s] for s in range(norm.shape[0])], axis=1)
    update[...] = jnp.dot(full, whole[...], preferred_element_type=jnp.float32)
    sums = jnp.concatenate([total[h] for h in range(total.shape[0])], axis=1)
    one, two = adam(sums, first[...], second[...])
    first_new[...] = one
    second_new[...] = two


def finish(norm, whole, total, first, second):
    parts, rows, shard = norm.shape
    ranks, depth = whole.shape
    halves = total.shape[0]
    block = first.shape[1]
    tile = tile_of(rows, 512)
    fp = jnp.float32
    by_rows = lambda i: (i, 0)
    deep = lambda i: (0, i, 0)
    return pl.pallas_call(
        finish_kernel,
        grid=(rows // tile,),
        out_shape=(
            jax.ShapeDtypeStruct((rows, depth), fp),
            jax.ShapeDtypeStruct((rows, block), fp),
            jax.ShapeDtypeStruct((rows, block), fp),
        ),
        in_specs=[
            pl.BlockSpec((parts, tile, shard), deep),
            pl.BlockSpec((ranks, depth), lambda i: (0, 0), pipeline_mode=pl.Buffered(1)),
            pl.BlockSpec((halves, tile, shard), deep),
            pl.BlockSpec((tile, block), by_rows),
            pl.BlockSpec((tile, block), by_rows),
        ],
        out_specs=(
            pl.BlockSpec((tile, depth), by_rows),
            pl.BlockSpec((tile, block), by_rows),
            pl.BlockSpec((tile, block), by_rows),
        ),
        compiler_params=pltpu.CompilerParams(vmem_limit_bytes=VMEM_LIMIT),
        name="finish",
    )(norm, whole, total, first, second)


def kernel_tile(size, fsdp, grad, projector_t, first):
    rows, depth = grad
    shard, block = projector_t[0], first[1]
    if size != 4 or fsdp < 2 or fsdp & (fsdp - 1):
        return 0
    if shard != LANES or block % shard or block * size != shard * fsdp or depth % LANES:
        return 0
    vmem = 2 * rows * depth + 2 * shard * fsdp * depth + rows * (3 * 4 * block + 2 * shard * fsdp + 12 * block)
    if vmem > VMEM_LIMIT * 0.92:
        return 0
    return tile_of(rows, 512)


def solution(mesh):
    size = mesh.shape["grp"]
    fsdp = mesh.shape["fsdp"]

    def step(grad, projector_t, first, second):
        tile = kernel_tile(size, fsdp, grad.shape, projector_t.shape, first.shape)
        if not tile:
            return plain_body(size, grad, projector_t, first, second)
        norm, total, whole = exchange(fsdp, tile, grad, projector_t, first, second)
        return finish(norm, whole, total, first, second)

    return jax.shard_map(
        step,
        mesh=mesh,
        in_specs=(P("fsdp", "grp"), P("fsdp", "grp"), P("fsdp", "grp"), P("fsdp", "grp")),
        out_specs=(P("fsdp", "grp"), P("fsdp", "grp"), P("fsdp", "grp")),
        check_vma=False,
    )
```

```python
import functools
import jax
import jax.numpy as jnp
from jax import lax
from jax.experimental import pallas as pl
from jax.experimental.pallas import tpu as pltpu
from jax.sharding import PartitionSpec as P

STEP = 10
CORRECT_ONE = 1.0 - 0.9**STEP
CORRECT_TWO = 1.0 - 0.999**STEP
MESH = pl.DeviceIdType.MESH
LANES = 128
EXCHANGE_LIMIT = 31100000
FINISH_LIMIT = 24000000
VMEM_ALL = 58600000


def flips(size):
    width = size.bit_length() - 1
    return [int(format(p, "b").zfill(width)[::-1], 2) if width else 0 for p in range(size)]


def swap(value, size, bit):
    return lax.ppermute(value, "grp", [(i, i ^ bit) for i in range(size)])


def pieces(rows):
    for count in (4, 2):
        if rows % (count * 8) == 0:
            return count
    return 1


def adam(total, first, second):
    one = 0.9 * first + 0.1 * total
    two = 0.999 * second + 0.001 * total * total
    return one, two


def normal(one, two):
    return (one * (1.0 / CORRECT_ONE) / (jnp.sqrt(two * (1.0 / CORRECT_TWO)) + 1e-08)).astype(jnp.bfloat16)


def plain_body(size, grad, projector_t, first_moment, second_moment):
    me = lax.axis_index("grp")
    whole = lax.all_gather(projector_t, "fsdp", axis=0, tiled=True)
    block = whole.shape[0] // size
    ranked = jnp.concatenate(
        [lax.dynamic_slice_in_dim(whole, (me ^ flip) * block, block, 0) for flip in flips(size)]
    )
    ranked = lax.optimization_barrier(ranked)
    rows = grad.shape[0]
    count = pieces(rows)
    step = rows // count
    bits = [1 << b for b in range(size.bit_length() - 1)]
    update = jnp.zeros((rows, grad.shape[1]), jnp.float32)
    first_new = jnp.zeros(first_moment.shape, jnp.float32)
    second_new = jnp.zeros(second_moment.shape, jnp.float32)
    for c in range(count):
        at = c * step
        part = lax.slice_in_dim(grad, at, at + step)
        half = ranked.shape[0] // 2
        total = None
        for n, bit in enumerate(bits):
            if n == 0:
                away = lax.dot_general(
                    part, ranked[half:], (((1,), (1,)), ((), ())), preferred_element_type=jnp.float32
                ).astype(jnp.bfloat16)
                total = lax.dot_general(
                    part, ranked[:half], (((1,), (1,)), ((), ())), preferred_element_type=jnp.float32
                )
            else:
                half = total.shape[1] // 2
                away = total[:, half:].astype(jnp.bfloat16)
                total = total[:, :half]
            total = total + swap(away, size, bit).astype(jnp.float32)
        one, two = adam(total, first_moment[at : at + step], second_moment[at : at + step])
        full = normal(one, two)
        first_new = lax.dynamic_update_slice_in_dim(first_new, one, at, 0)
        second_new = lax.dynamic_update_slice_in_dim(second_new, two, at, 0)
        for bit in reversed(bits):
            full = jnp.concatenate([full, swap(full, size, bit)], axis=1)
        out = jnp.dot(full, ranked, preferred_element_type=jnp.float32)
        update = lax.dynamic_update_slice_in_dim(update, out, at, 0)
    return (update, first_new, second_new)


def tile_of(rows, most):
    for t in range(most - most % 16, 0, -16):
        if rows % t == 0:
            return t
    return 0


def xor(a, b, bits):
    out = 0
    for i in range(bits):
        p = 1 << i
        out = out + ((a // p + b // p) % 2) * p
    return out


LAG_B, LAG_C, LAG_D, LAG_E, LAG_F = 2, 5, 8, 9, 10
SLOTS = LAG_C - LAG_B + 1
CHUNKS = 2
FORWARD = ((9, 11), (18, 22), (30, 36))
MIDDLE_SEND = 6
LATE_SEND = 18


def exchange_kernel(
    fsdp, tile, kept,
    grad_hbm, proj_hbm, first_hbm, second_hbm,
    norm, whole, first, second, early,
    grad, ring, away, near, cross, came,
    load_sem, grad_sem, mom_sem,
    p_send, p_recv, d_send, d_recv, y_send, y_recv, ny_send, nd_send, n_recv,
):
    f = lax.axis_index("fsdp")
    g = lax.axis_index("grp")
    y, c = g // 2, g % 2
    shard = proj_hbm.shape[0]
    _, rows, _ = first.shape
    tiles = rows // tile
    half = tile // 2
    bits = fsdp.bit_length() - 1
    single = 4 * tiles
    steps = fsdp * tiles
    x_to = xor(f, 1, bits)
    core_to = y * 2 + (1 - c)
    y_to = (1 - y) * 2 + c
    bf, fp = jnp.bfloat16, jnp.float32

    own = pltpu.make_async_copy(
        proj_hbm, whole.at[pl.ds(pl.multiple_of(f * shard, shard), shard)], load_sem
    )
    own.start()

    def grad_copy(j):
        at = pl.ds(pl.multiple_of(j * tile, tile), tile)
        return pltpu.make_async_copy(grad_hbm.at[at], grad.at[at], grad_sem.at[j])

    def mom_copies():
        out = []
        for i, (src, dst) in enumerate(((first_hbm, first), (second_hbm, second))):
            for h in range(2):
                out.append(
                    pltpu.make_async_copy(
                        src.at[:, pl.ds(h * shard, shard)], dst.at[h], mom_sem.at[i, h]
                    )
                )
        return out

    grad_copy(0).start()

    barrier = pltpu.get_barrier_semaphore()
    peers = [(x_to, g), (f, core_to), (f, y_to)]
    peers += [(xor(f, 2 * m, bits), g) for m in range(1, fsdp // 2)]
    for peer in peers:
        pl.semaphore_signal(barrier, inc=1, device_id=peer, device_id_type=MESH)

    @pl.loop(1, tiles)
    def _(j):
        grad_copy(j).start()

    for copy in mom_copies():
        copy.start()
    pl.semaphore_wait(barrier, len(peers))
    own.wait()

    def p_copy(sid, q, to):
        size = shard // CHUNKS
        ref = whole.at[pl.ds(pl.multiple_of(sid * shard + q * size, size), size)]
        return pltpu.make_async_remote_copy(
            ref, ref, p_send, p_recv.at[sid, q], device_id=(to, g), device_id_type=MESH
        )

    def p_give(to):
        for q in range(CHUNKS):
            p_copy(f, q, to).start()

    def p_take(k):
        for q in range(CHUNKS):
            p_copy(xor(f, k, bits), q, x_to).wait_recv()

    p_give(x_to)
    p_give(xor(f, 2, bits))

    bit_0, bit_1 = f % 2, (f // 2) % 2
    far = xor(f // 2, 2, bits - 1)
    far_0 = far % 2
    two = jnp.int32(2)

    def place(s, width):
        if width == 1:
            k = lax.div(s, jnp.int32(tiles))
            j = s - k * tiles
            k_1 = lax.div(k, two)
            k_0 = k - 2 * k_1
            base = f + k - 2 * (bit_0 * k_0 + 2 * bit_1 * k_1)
            block = lax.div(base, two)
            h = base - 2 * block
            size = tile
        else:
            s = s - single
            k = lax.div(s, jnp.int32(2 * tiles))
            j = s - k * (2 * tiles)
            block = far + k - 2 * far_0 * k
            base = 2 * block
            h = 0
            size = half
        line = lax.div(block, two)
        return k, j, pl.multiple_of(j * size, size), size, base, line, block - 2 * line, h

    def product(base, at, width, size):
        return lax.dot_general(
            grad[pl.ds(at, size)],
            whole[pl.ds(pl.multiple_of(base * shard, shard), shard * width)],
            (((1,), (1,)), ((), ())),
            preferred_element_type=fp,
        )

    def piece(ref, lead, at, width, size):
        return ref.at[pl.ds(lead, width), pl.ds(at, size)]

    def d_copy(s, slot, at, width, size):
        return pltpu.make_async_remote_copy(
            piece(away, slot, at, width, size), piece(near, slot, at, width, size),
            d_send, d_recv.at[s], device_id=(f, core_to), device_id_type=MESH,
        )

    def y_copy(s, h, at, width, size):
        return pltpu.make_async_remote_copy(
            piece(cross, h, at, width, size), piece(came, h, at, width, size),
            y_send, y_recv.at[s], device_id=(f, y_to), device_id_type=MESH,
        )

    def n_copy(s, base, at, width, size, send, to):
        ref = piece(norm, base, at, width, size)
        return pltpu.make_async_remote_copy(
            ref, ref, send, n_recv.at[s], device_id=(f, to), device_id_type=MESH
        )

    def give(s, width):
        k, j, at, size, base, line, side, h = place(s, width)

        @pl.when(side != c)
        def _():
            slot = line * 2 + h
            part = product(base, at, width, size).astype(bf)
            for i in range(width):
                away[slot + i, pl.ds(at, size)] = part[:, i * shard : (i + 1) * shard]
            d_copy(s, slot, at, width, size).start()

    def keep(s, width):
        k, j, at, size, base, line, side, h = place(s, width)

        @pl.when(side == c)
        def _():
            slot = line * 2 + h
            part = product(base, at, width, size)
            d_copy(s, slot, at, width, size).wait_recv()
            sums = [
                part[:, i * shard : (i + 1) * shard] + near[slot + i, pl.ds(at, size)].astype(fp)
                for i in range(width)
            ]

            @pl.when(line != y)
            def _():
                for i in range(width):
                    cross[h + i, pl.ds(at, size)] = sums[i].astype(bf)
                y_copy(s, h, at, width, size).start()

            @pl.when(line == y)
            def _():
                for i in range(width):
                    ring[lax.rem(s, jnp.int32(SLOTS)), pl.ds(i * size, size)] = sums[i]

    def own_step(s, width):
        k, j, at, size, base, line, side, h = place(s, width)

        @pl.when((line == y) & (side == c))
        def _():
            y_copy(s, h, at, width, size).wait_recv()
            here = pl.ds(at, size)
            for i in range(width):
                full = ring[lax.rem(s, jnp.int32(SLOTS)), pl.ds(i * size, size)] + came[h + i, here].astype(fp)
                one, two = adam(full, first[h + i, here], second[h + i, here])
                first[h + i, here] = one
                second[h + i, here] = two
                norm[base + i, here] = normal(one, two)
            n_copy(s, base, at, width, size, ny_send, y_to).start()
            n_copy(s, base, at, width, size, nd_send, core_to).start()

    def hand(s, width):
        k, j, at, size, base, line, side, h = place(s, width)

        @pl.when((side == c) & (line != y))
        def _():
            copy = n_copy(s, base, at, width, size, nd_send, core_to)
            copy.wait_recv()
            copy.start()

    def take(s, width):
        k, j, at, size, base, line, side, h = place(s, width)

        @pl.when(side != c)
        def _():
            n_copy(s, base, at, width, size, nd_send, core_to).wait_recv()

    def spread(s, width):
        k, j, at, size, base, line, side, h = place(s, width)
        lead = line * 4 + side * 2

        def add(fresh):
            here = pl.ds(at, size)
            left = jnp.concatenate([norm[lead, here], norm[lead + 1, here]], axis=1)
            right = pl.ds(pl.multiple_of(lead * shard, shard), 2 * shard)
            depth = whole.shape[1]
            cut = depth // 2 if depth % (2 * LANES) == 0 else depth
            for n in range(0, depth, cut):
                out = jnp.dot(left, whole[right, n : n + cut], preferred_element_type=fp)
                if fresh:
                    early[here, n : n + cut] = out
                else:
                    early[here, n : n + cut] += out

        inside = j * size < kept
        if width == 1:
            pl.when(inside & (k == 1))(lambda: add(True))
            pl.when(inside & (k == 3))(lambda: add(False))
        else:
            pl.when(inside)(lambda: add(False))

    def phase(t, lag, run):
        s = t - lag
        pl.when((s >= 0) & (s < single))(lambda: run(s, 1))
        pl.when((s >= single) & (s < steps))(lambda: run(s, 2))

    def step(t, carry):
        @pl.when(t < tiles)
        def _():
            grad_copy(t).wait()

        pl.when(t == MIDDLE_SEND)(lambda: p_give(xor(f, 4, bits)))
        pl.when(t == LATE_SEND)(lambda: p_give(xor(f, 6, bits)))
        for m, times in enumerate(FORWARD):
            for q, when in enumerate(times):

                @pl.when(t == when)
                def _():
                    sid = xor(f, 2 * (m + 1), bits)
                    p_copy(sid, q, x_to).wait_recv()
                    p_copy(sid, q, x_to).start()

        for k, when in ((1, tiles), (3, 3 * tiles), (5, 4 * tiles), (7, 6 * tiles)):
            pl.when(t == when)(lambda: p_take(k))

        phase(t, LAG_D, hand)
        phase(t, LAG_B, keep)
        phase(t, 0, give)

        @pl.when(t == LAG_C)
        def _():
            for copy in mom_copies():
                copy.wait()

        phase(t, LAG_C, own_step)
        phase(t, LAG_E, take)
        phase(t, LAG_F, spread)
        return carry

    lax.fori_loop(0, steps + LAG_F, step, 0)

    def sent(ref, sem):
        pltpu.make_async_remote_copy(
            ref, ref, sem, n_recv.at[0], device_id=(f, y_to), device_id_type=MESH
        ).wait_send()

    sent(whole.at[pl.ds(0, (fsdp - 1) * shard)], p_send)
    sent(away, d_send)
    sent(cross, y_send)
    sent(cross, ny_send)
    sent(away, nd_send)


def exchange(fsdp, tile, kept, grad, projector_t, first, second):
    rows, depth = grad.shape
    shard = projector_t.shape[0]
    ranks = shard * fsdp
    tiles = rows // tile
    steps = fsdp * tiles
    bf, fp = jnp.bfloat16, jnp.float32
    sem = pltpu.SemaphoreType.DMA
    return pl.pallas_call(
        functools.partial(exchange_kernel, fsdp, tile, kept),
        out_shape=(
            pltpu.VMEM((fsdp, rows, shard), bf),
            pltpu.VMEM((ranks, depth), bf),
            pltpu.VMEM((2, rows, shard), fp),
            pltpu.VMEM((2, rows, shard), fp),
            pltpu.VMEM((kept, depth), fp),
        ),
        in_specs=[pl.BlockSpec(memory_space=pl.ANY)] * 4,
        out_specs=(pl.BlockSpec(memory_space=pltpu.VMEM),) * 5,
        scratch_shapes=[
            pltpu.VMEM((rows, depth), bf),
            pltpu.VMEM((SLOTS, tile, shard), fp),
            pltpu.VMEM((4, rows, shard), bf),
            pltpu.VMEM((4, rows, shard), bf),
            pltpu.VMEM((2, rows, shard), bf),
            pltpu.VMEM((2, rows, shard), bf),
            sem(()),
            sem((tiles,)),
            sem((2, 2)),
            sem(()),
            sem((fsdp, CHUNKS)),
            sem(()),
            sem((steps,)),
            sem(()),
            sem((steps,)),
            sem(()),
            sem(()),
            sem((steps,)),
        ],
        compiler_params=pltpu.CompilerParams(
            collective_id=0, has_side_effects=True, vmem_limit_bytes=EXCHANGE_LIMIT
        ),
        name="exchange",
    )(grad, projector_t, first, second)


def finish_kernel(
    tile, norm, whole, first, second, early, update, first_new, second_new, held, sems, mom_sems
):
    shard = first.shape[2]
    kept = early.shape[0]
    tiles = held.shape[0]
    moved = []
    for i, (src, dst) in enumerate(((first, first_new), (second, second_new))):
        for h in range(2):
            moved.append(
                pltpu.make_async_copy(src.at[h], dst.at[:, pl.ds(h * shard, shard)], mom_sems.at[i, h])
            )
    count = kept // tile
    for i in range(count):
        part = pl.ds(i * tile, tile)
        moved.append(pltpu.make_async_copy(early.at[part], update.at[part], sems.at[tiles + i]))
    for copy in moved:
        copy.start()

    def out(i):
        at = pl.ds(pl.multiple_of(kept + i * tile, tile), tile)
        return pltpu.make_async_copy(held.at[i], update.at[at], sems.at[i])

    @pl.loop(0, tiles)
    def _(i):
        at = pl.ds(pl.multiple_of(kept + i * tile, tile), tile)
        full = jnp.concatenate([norm[s, at] for s in range(norm.shape[0])], axis=1)
        held[i] = jnp.dot(full, whole[...], preferred_element_type=jnp.float32)
        out(i).start()

    @pl.loop(0, tiles)
    def _(i):
        out(i).wait()

    for copy in moved:
        copy.wait()


def finish(tile, norm, whole, first, second, early):
    parts, rows, shard = norm.shape
    ranks, depth = whole.shape
    kept = early.shape[0]
    block = 2 * shard
    tiles = (rows - kept) // tile
    fp = jnp.float32
    inside = pl.BlockSpec(memory_space=pltpu.VMEM)
    outside = pl.BlockSpec(memory_space=pl.ANY)
    return pl.pallas_call(
        functools.partial(finish_kernel, tile),
        out_shape=(
            jax.ShapeDtypeStruct((rows, depth), fp),
            jax.ShapeDtypeStruct((rows, block), fp),
            jax.ShapeDtypeStruct((rows, block), fp),
        ),
        in_specs=[inside] * 5,
        out_specs=(outside,) * 3,
        scratch_shapes=[
            pltpu.VMEM((tiles, tile, depth), fp),
            pltpu.SemaphoreType.DMA((tiles + kept // tile,)),
            pltpu.SemaphoreType.DMA((2, 2)),
        ],
        compiler_params=pltpu.CompilerParams(vmem_limit_bytes=FINISH_LIMIT),
        name="finish",
    )(norm, whole, first, second, early)


def plan(size, fsdp, grad, projector_t, first):
    rows, depth = grad
    shard, block = projector_t[0], first[1]
    if size != 4 or fsdp != 2 * size or shard != LANES or block != 2 * shard or depth % LANES:
        return None
    tile = tile_of(rows, 512)
    if tile < 256 or tile % 32 or rows // tile < LAG_C:
        return None
    scratch = 2 * rows * depth + SLOTS * tile * shard * 4 + 12 * rows * block
    if scratch > EXCHANGE_LIMIT - (1 << 20):
        return None
    room = VMEM_ALL - EXCHANGE_LIMIT - 2 * shard * fsdp * (rows + depth) - 8 * rows * block
    kept = room // (4 * depth * tile) * tile
    if kept < tile or kept >= rows or (rows - kept) * depth * 4 > FINISH_LIMIT - (1 << 21):
        return None
    return tile, kept


def solution(mesh):
    size = mesh.shape["grp"]
    fsdp = mesh.shape["fsdp"]

    def step(grad, projector_t, first, second):
        sizes = plan(size, fsdp, grad.shape, projector_t.shape, first.shape)
        if sizes is None:
            return plain_body(size, grad, projector_t, first, second)
        tile, kept = sizes
        norm, whole, first, second, early = exchange(fsdp, tile, kept, grad, projector_t, first, second)
        return finish(tile // 2, norm, whole, first, second, early)

    return jax.shard_map(
        step,
        mesh=mesh,
        in_specs=(P("fsdp", "grp"), P("fsdp", "grp"), P("fsdp", "grp"), P("fsdp", "grp")),
        out_specs=(P("fsdp", "grp"), P("fsdp", "grp"), P("fsdp", "grp")),
        check_vma=False,
    )
```
